16 devices in a mesh: tp: 2 (over z), dp: 8 (over y, x, core).
Axes of the slice: x: 2, y: 2, z: 2, core: 2. Of those that a mesh axis runs over, the one named last changes fastest.
Arguments:
- hidden: bfloat16 [24, 256, 896], P('dp')
- labels: int32 [24, 256], P('dp')
- loss_mask: int32 [24, 256], P('dp')
- norm_gain: bfloat16 [896], replicated
- embed_table: bfloat16 [151936, 896], P('tp')
Outputs:
- output 1: float32 [], replicated
- output 2: float32 [24, 256, 896], P('dp')
- output 3: float32 [151936, 896], P('tp', 'dp')
- output 4: float32 [896], replicated
All inputs are finite; a program needn't handle non-finite values.
Results may differ from the reference program's by a relative error of at most 0.001.
Values sent between devices are 32-bit elements.
A program may use at most 1 GiB of HBM per device.

```python
import jax
import jax.numpy as jnp
from jax import lax

VOCAB = 151936
HIDDEN = 896
BATCH = 24
SEQ_LEN = 256
EPSILON = 1e-6
ROW_BLOCK = min(SEQ_LEN, 128)


def draw_mask(key_start, key_len):
    run_start = jax.random.randint(key_start, (BATCH, 1), 0, SEQ_LEN // 2, jnp.int32)
    run_stop = run_start + 1 + jax.random.randint(key_len, (BATCH, 1), 0, SEQ_LEN - run_start, jnp.int32)
    positions = jnp.arange(SEQ_LEN, dtype=jnp.int32)[None, :]
    return ((positions >= run_start) & (positions < run_stop)).astype(jnp.int32)


def setup_inputs(seed: int = 0) -> dict:
    base_key = jax.random.key(seed)
    key_hid, key_lab, key_start, key_len, key_gain, key_table = jax.random.split(base_key, 6)
    hidden = jax.random.normal(key_hid, (BATCH, SEQ_LEN, HIDDEN), jnp.float32).astype(jnp.bfloat16)
    labels = jax.random.randint(key_lab, (BATCH, SEQ_LEN), 0, VOCAB, jnp.int32)
    loss_mask = draw_mask(key_start, key_len)
    norm_gain = (1.0 + 0.25 * jax.random.normal(key_gain, (HIDDEN,), jnp.float32)).astype(jnp.bfloat16)
    embed_table = (2.5 * HIDDEN ** -0.5 * jax.random.normal(key_table, (VOCAB, HIDDEN), jnp.float32)).astype(jnp.bfloat16)
    return {"hidden": hidden, "labels": labels, "loss_mask": loss_mask, "norm_gain": norm_gain, "embed_table": embed_table}


def reference(hidden, labels, loss_mask, norm_gain, embed_table):
    n_block = BATCH * SEQ_LEN // ROW_BLOCK
    hid_all = hidden.reshape(n_block, ROW_BLOCK, HIDDEN)
    lab_all = labels.reshape(n_block, ROW_BLOCK)
    mask_all = loss_mask.astype(jnp.float32).reshape(n_block, ROW_BLOCK)
    mask_count = jnp.sum(mask_all)
    gain32 = norm_gain.astype(jnp.float32)
    vocab_ids = jnp.arange(VOCAB)

    def block_step(carry_in, block_in):
        loss_sum, grad_embed, grad_gain = carry_in
        hid_blk, lab_blk, mask_blk = block_in
        x_full = hid_blk.astype(jnp.float32)
        inv_rms = lax.rsqrt(jnp.mean(x_full * x_full, axis=-1, keepdims=True) + EPSILON)
        x_hat = x_full * inv_rms
        normed = (x_hat * gain32).astype(jnp.bfloat16)
        logits = jnp.dot(normed, embed_table.T, preferred_element_type=jnp.float32)
        log_norm = jax.nn.logsumexp(logits, axis=-1)
        one_hot = (vocab_ids[None, :] == lab_blk[:, None]).astype(jnp.float32)
        target = jnp.sum(one_hot * logits, axis=-1)
        loss_sum = loss_sum + jnp.sum(mask_blk * (log_norm - target))
        softmax = jnp.exp(logits - log_norm[:, None])
        grad_logit = ((softmax - one_hot) * (mask_blk / mask_count)[:, None]).astype(jnp.bfloat16)
        grad_norm = jnp.dot(grad_logit, embed_table, preferred_element_type=jnp.float32)
        grad_gain = grad_gain + jnp.sum(grad_norm * x_hat, axis=0)
        grad_xhat = grad_norm * gain32
        grad_hid = inv_rms * (grad_xhat - x_hat * jnp.mean(grad_xhat * x_hat, axis=-1, keepdims=True))
        grad_embed = grad_embed + jnp.dot(grad_logit.T, normed, preferred_element_type=jnp.float32)
        return (loss_sum, grad_embed, grad_gain), grad_hid

    init_carry = (jnp.zeros((), jnp.float32), jnp.zeros((VOCAB, HIDDEN), jnp.float32), jnp.zeros((HIDDEN,), jnp.float32))
    (loss_sum, grad_embed, grad_gain), grad_all = lax.scan(block_step, init_carry, (hid_all, lab_all, mask_all))
    return loss_sum / mask_count, grad_all.reshape(BATCH, SEQ_LEN, HIDDEN), grad_embed, grad_gain
```

```python
import functools

import jax
import jax.numpy as jnp
from jax import lax
from jax.experimental import pallas as pl
from jax.experimental.pallas import tpu as pltpu
from jax.sharding import PartitionSpec as P


EPSILON = 1e-6
NEG = -1e30
VB = 256
NT = (((1,), (1,)), ((), ()))

CHUNKS = (2, 6, 5, 6)


def logit_kernel(vocab_loc, nblk, first, d_ref, *refs):
    pieces, (off_ref, gain_ref, e_ref), rest = refs[:2], refs[2:5], refs[5:]
    if first:
        z_ref, ut_ref, lab_ref, st_ref, eo_ref, u_s, m_s, s_s, t_s, l_s = rest
    else:
        _, _, _, z_ref, ut_ref, lab_ref, st_ref, u_s, m_s, s_s, t_s, l_s = rest
    j = pl.program_id(0)
    steps, width = nblk // 2, 2 * VB
    half = u_s.shape[0] // 2
    base = (d_ref[0] * nblk + 2 * j) * VB

    @pl.when(j == 0)
    def _():
        for part, h_ref in enumerate(pieces):
            for i in range(half // 256):
                x = h_ref[i * 256:(i + 1) * 256, :]
                r = lax.rsqrt(jnp.mean(x * x, axis=-1, keepdims=True) + EPSILON)
                y = ((x * r) * gain_ref[...]).astype(jnp.bfloat16)
                at = part * half + i * 256
                u_s[at:at + 256, :] = y
                ut_ref[:, at:at + 256] = y.T
            row = h_ref[half:half + 8, :][:1, :half].astype(jnp.int32) - off_ref[0]
            row = jnp.where(row < vocab_loc, row, -1)
            lab_ref[part * half:(part + 1) * half, :] = jnp.broadcast_to(row, (128, half)).T
        m_s[...] = jnp.full(m_s.shape, NEG, jnp.float32)
        s_s[...] = jnp.zeros(s_s.shape, jnp.float32)
        t_s[...] = jnp.zeros(t_s.shape, jnp.float32)
        l_s[...] = lab_ref[...] - lax.broadcasted_iota(jnp.int32, lab_ref.shape, 1)

    if first:
        rows = lax.broadcasted_iota(jnp.int32, e_ref.shape, 0) + base
        eo_ref[...] = jnp.where(rows < vocab_loc, e_ref[...].astype(jnp.float32), 0.0).astype(jnp.bfloat16)
        e_ref = eo_ref
    bias = jnp.where(lax.broadcasted_iota(jnp.int32, (1, width), 1) + base < vocab_loc, 0.0, NEG)
    for i in range(2 * half // 256):
        sl = slice(i * 256, (i + 1) * 256)
        z = lax.dot_general(u_s[sl, :], e_ref[...], NT, preferred_element_type=jnp.float32) + bias
        z_ref[0, sl, :] = z[:, :VB]
        z_ref[1, sl, :] = z[:, VB:]
        parts = [z[:, k:k + 128] for k in range(0, width, 128)]
        m_old = m_s[sl, :]
        m_new = functools.reduce(jnp.maximum, parts, m_old)
        m_s[sl, :] = m_new
        s_s[sl, :] = s_s[sl, :] * jnp.exp(m_old - m_new) + sum(jnp.exp(p - m_new) for p in parts)
        lab, target = l_s[sl, :], t_s[sl, :]
        for k, p in enumerate(parts):
            target = jnp.where(lab == base + k * 128, p, target)
        t_s[sl, :] = target

    @pl.when(j == steps - 1)
    def _():
        m_all = jnp.max(m_s[...], axis=-1, keepdims=True)
        s_all = jnp.sum(s_s[...] * jnp.exp(m_s[...] - m_all), axis=-1, keepdims=True)
        t_all = jnp.sum(t_s[...], axis=-1, keepdims=True)
        lane = lax.broadcasted_iota(jnp.int32, m_s.shape, 1)
        st_ref[...] = jnp.where(lane == 0, m_all, jnp.where(lane == 1, s_all, t_all)).T[:8, :]
        for part, h_ref in enumerate(pieces):
            st_ref[3:4, part * half:(part + 1) * half] = h_ref[half:half + 8, :][1:2, :half]


def logits_call(group, n_group, vocab_loc, nblk, half, dev, ha, hb, off, gain, embed, prev):
    ext, hid = ha.shape
    tg, width, steps = 2 * half, 2 * VB, nblk // 2
    first = prev is None
    last = (vocab_loc + width - 1) // width - 1
    one = pl.Buffered(1)
    if first:
        e_map = lambda j, d: (jnp.minimum(d[0] * steps + j, last), 0)
    else:
        e_map = lambda j, d: (j, 0)
    in_specs = [
        pl.BlockSpec((ext, hid), lambda j, d: (0, 0), pipeline_mode=one),
        pl.BlockSpec((ext, hid), lambda j, d: (0, 0), pipeline_mode=one),
        pl.BlockSpec(memory_space=pltpu.SMEM),
        pl.BlockSpec((1, hid), lambda j, d: (0, 0)),
        pl.BlockSpec((width, hid), e_map),
    ]
    out_specs = [
        pl.BlockSpec((2, tg, VB), lambda j, d: (j, group, 0)),
        pl.BlockSpec((hid, tg), lambda j, d: (0, group)),
        pl.BlockSpec((tg, 128), lambda j, d: (group, 0)),
        pl.BlockSpec((8, tg), lambda j, d: (0, 0)),
    ]
    out_shape = [
        jax.ShapeDtypeStruct((nblk, n_group * tg, VB), jnp.float32),
        jax.ShapeDtypeStruct((hid, n_group * tg), jnp.bfloat16),
        jax.ShapeDtypeStruct((n_group * tg, 128), jnp.int32),
        jax.ShapeDtypeStruct((8, tg), jnp.float32),
    ]
    args = [dev, ha, hb, off, gain, embed]
    alias = {}
    if first:
        out_specs.append(pl.BlockSpec((width, hid), lambda j, d: (j, 0)))
        out_shape.append(jax.ShapeDtypeStruct((nblk * VB, hid), jnp.bfloat16))
    else:
        in_specs += [pl.BlockSpec(memory_space=pl.ANY)] * 3
        alias = {6: 0, 7: 1, 8: 2}
        args += list(prev)
    return pl.pallas_call(
        functools.partial(logit_kernel, vocab_loc, nblk, first),
        grid_spec=pltpu.PrefetchScalarGridSpec(
            num_scalar_prefetch=1,
            grid=(steps,),
            in_specs=in_specs,
            out_specs=out_specs,
            scratch_shapes=[
                pltpu.VMEM((tg, hid), jnp.bfloat16),
                pltpu.VMEM((tg, 128), jnp.float32),
                pltpu.VMEM((tg, 128), jnp.float32),
                pltpu.VMEM((tg, 128), jnp.float32),
                pltpu.VMEM((tg, 128), jnp.int32),
            ],
        ),
        out_shape=out_shape,
        input_output_aliases=alias,
        compiler_params=pltpu.CompilerParams(vmem_limit_bytes=60 << 20),
        cost_estimate=pl.CostEstimate(flops=2 * tg * nblk * VB * hid, bytes_accessed=4 * tg * nblk * VB, transcendentals=0),
        name="logits",
    )(*args)


def grad_block(z, lse, wgt, lab, base):
    parts = []
    for k in range(VB // 128):
        p = jnp.exp(z[:, k * 128:(k + 1) * 128] - lse)
        p = jnp.where(lab == base + k * 128, p - 1.0, p)
        parts.append((p * wgt).astype(jnp.bfloat16))
    return jnp.concatenate(parts, axis=1)


def hidden_grad_kernel(nblk, inner, n_out, d_ref, z_ref, lse_ref, w_ref, lab_ref, e_ref, *rest):
    lse, wgt = lse_ref[...], w_ref[...]
    lab = lab_ref[...] - lax.broadcasted_iota(jnp.int32, lab_ref.shape, 1)
    acc_s, outs = rest[-1], rest[-1 - n_out:-1]
    acc_s[...] = rest[0][...] if len(rest) > n_out + 1 else jnp.zeros(acc_s.shape, jnp.float32)

    def step(it, carry):
        acc = None
        for k in range(inner):
            j = it * inner + k
            g = grad_block(z_ref[j], lse, wgt, lab, (d_ref[0] * nblk + j) * VB)
            e = e_ref[pl.ds(pl.multiple_of(j * VB, VB), VB), :]
            part = jnp.dot(g, e, preferred_element_type=jnp.float32)
            acc = part if acc is None else acc + part
        acc_s[...] += acc
        return carry

    lax.fori_loop(0, nblk // inner, step, 0)
    if n_out == 1:
        outs[0][...] = acc_s[...]
    else:
        per = pl.num_programs(0) // n_out
        for c in range(n_out):
            @pl.when(pl.program_id(0) // per == c)
            def _():
                outs[c][...] = acc_s[...]


def hidden_grad(dev, z, lse, wgt, lab, e_dev, parity, n_slot, add=None):
    nblk, tokens, _ = z.shape
    hid = e_dev.shape[1]
    tb = 256
    per = tokens // n_slot // tb
    steps = n_slot // 2 * per
    n_out = 1 if add is None else n_slot // 2
    at = lambda i: (2 * (i // per) + parity) * per + i % per
    wide = pl.BlockSpec((tb, 128), lambda i, d: (at(i), 0))
    in_specs = [
        pl.BlockSpec((nblk, tb, VB), lambda i, d: (0, at(i), 0)),
        wide, wide, wide,
        pl.BlockSpec((nblk * VB, hid), lambda i, d: (0, 0), pipeline_mode=pl.Buffered(1)),
    ]
    args = [dev, z, lse, wgt, lab, e_dev]
    row = pl.BlockSpec((tb, hid), lambda i, d: (i, 0))
    if add is None:
        out_specs = [row]
        out_shape = [jax.ShapeDtypeStruct((steps * tb, hid), jnp.float32)]
    else:
        in_specs.append(row)
        args.append(add)
        out_specs = [
            pl.BlockSpec((tb, hid), functools.partial(lambda c, i, d: (jnp.clip(i - c * per, 0, per - 1), 0), c))
            for c in range(n_out)
        ]
        out_shape = [jax.ShapeDtypeStruct((per * tb, hid), jnp.float32)] * n_out
    return pl.pallas_call(
        functools.partial(hidden_grad_kernel, nblk, 19, n_out),
        grid_spec=pltpu.PrefetchScalarGridSpec(
            num_scalar_prefetch=1,
            grid=(steps,),
            in_specs=in_specs,
            out_specs=out_specs,
            scratch_shapes=[pltpu.VMEM((tb, hid), jnp.float32)],
        ),
        out_shape=out_shape,
        compiler_params=pltpu.CompilerParams(vmem_limit_bytes=60 << 20),
        cost_estimate=pl.CostEstimate(flops=tokens * nblk * VB * hid, bytes_accessed=2 * tokens * nblk * VB, transcendentals=0),
        name="hidden_grad",
    )(*args)


def embed_grad_kernel(nblk, off, n_dp, d_ref, z_ref, lse_ref, w_ref, lab_ref, ut_ref, *rest):
    outs, acc_s = rest[:n_dp], rest[n_dp]
    j = pl.program_id(0)
    hid, tokens = ut_ref.shape
    cols = hid // n_dp
    lane = lax.broadcasted_iota(jnp.int32, (256, 128), 1)
    acc = None
    for i in range(tokens // 256):
        sl = slice(i * 256, (i + 1) * 256)
        lse, wgt, lab = lse_ref[sl, :], w_ref[sl, :], lab_ref[sl, :] - lane
        g = jnp.concatenate(
            [grad_block(z_ref[k, sl, :], lse, wgt, lab, (d_ref[0] * nblk + (off + j) * 2 + k) * VB) for k in range(2)],
            axis=1,
        )
        part = jnp.dot(ut_ref[:, sl], g, preferred_element_type=jnp.float32)
        acc = part if acc is None else acc + part
    acc_s[...] = acc
    for r in range(n_dp):
        at = pl.multiple_of((d_ref[0] ^ r) * cols, 8)
        outs[r][...] = acc_s[pl.ds(at, cols), :]


def embed_grad(dev, z, lse, wgt, lab, ut, off, steps, n_dp):
    nblk, tokens, _ = z.shape
    hid = ut.shape[0]
    cols = hid // n_dp
    one = pl.Buffered(1)
    wide = pl.BlockSpec((tokens, 128), lambda j, d: (0, 0), pipeline_mode=one)
    return pl.pallas_call(
        functools.partial(embed_grad_kernel, nblk, off, n_dp),
        grid_spec=pltpu.PrefetchScalarGridSpec(
            num_scalar_prefetch=1,
            grid=(steps,),
            in_specs=[
                pl.BlockSpec((2, tokens, VB), lambda j, d: (off + j, 0, 0)),
                wide, wide, wide,
                pl.BlockSpec((hid, tokens), lambda j, d: (0, 0), pipeline_mode=one),
            ],
            out_specs=[pl.BlockSpec((cols, 2 * VB), lambda j, d: (0, j))] * n_dp,
            scratch_shapes=[pltpu.VMEM((hid, 2 * VB), jnp.float32)],
        ),
        out_shape=[jax.ShapeDtypeStruct((cols, steps * 2 * VB), jnp.float32)] * n_dp,
        compiler_params=pltpu.CompilerParams(vmem_limit_bytes=60 << 20),
        cost_estimate=pl.CostEstimate(flops=2 * tokens * steps * 2 * VB * hid, bytes_accessed=8 * tokens * steps * VB, transcendentals=0),
        name="embed_grad",
    )(dev, z, lse, wgt, lab, ut)


def place_kernel(n_dp, per, off, last, d_ref, *refs):
    pieces, out = refs[:n_dp], refs[-1]
    s, j = pl.program_id(0), pl.program_id(1)
    for r in range(n_dp):
        @pl.when(((s ^ d_ref[0]) == r) & (s * per + off + j <= last))
        def _():
            out[...] = pieces[r][...]


def place(dev, pieces, prev, off, steps, vocab_loc, nblk):
    n_dp, cols = len(pieces), pieces[0].shape[0]
    rows, per = 2 * VB, nblk // 2
    last = (vocab_loc + rows - 1) // rows - 1
    specs = [
        pl.BlockSpec((cols, rows), functools.partial(lambda r, s, j, d: (0, jnp.where((s ^ d[0]) == r, j, 0)), r))
        for r in range(n_dp)
    ]
    args = [dev, *pieces]
    alias = {}
    if prev is not None:
        specs.append(pl.BlockSpec(memory_space=pl.ANY))
        args.append(prev)
        alias = {n_dp + 1: 0}
    return pl.pallas_call(
        functools.partial(place_kernel, n_dp, per, off, last),
        grid_spec=pltpu.PrefetchScalarGridSpec(
            num_scalar_prefetch=1,
            grid=(n_dp, steps),
            in_specs=specs,
            out_specs=pl.BlockSpec((cols, rows), lambda s, j, d: (0, jnp.minimum(s * per + off + j, last))),
        ),
        out_shape=jax.ShapeDtypeStruct((cols, vocab_loc), jnp.float32),
        input_output_aliases=alias,
        cost_estimate=pl.CostEstimate(flops=n_dp * steps * rows * cols, bytes_accessed=8 * n_dp * steps * rows * cols, transcendentals=0),
        name="place",
    )(*args)


def solution(mesh):
    n_dp, n_tp = mesh.shape["dp"], mesh.shape["tp"]

    def swap(x, mask, axis="dp"):
        size = n_dp if axis == "dp" else n_tp
        return lax.ppermute(x, axis, [(i, i ^ mask) for i in range(size)])

    def local_step(hidden, labels, loss_mask, norm_gain, embed_table):
        n_seq, seq_len, hid = hidden.shape
        vocab_loc = embed_table.shape[0]
        tokens = n_seq * seq_len
        unit = 2 * VB * n_dp
        nblk = (vocab_loc + unit - 1) // unit * 2
        me = lax.axis_index("dp").astype(jnp.int32)
        dev = me.reshape(1)
        offset = lax.axis_index("tp").astype(jnp.int32) * vocab_loc
        n_chip = n_dp // 2

        x_full = hidden.reshape(tokens, hid).astype(jnp.float32)
        gain32 = norm_gain.astype(jnp.float32)
        ints = jnp.stack([labels.reshape(tokens), loss_mask.reshape(tokens)]).astype(jnp.float32)
        mine = jnp.concatenate([x_full, jnp.pad(ints, ((0, 6), (0, hid - tokens)))])
        held = [mine] + [swap(mine, 2 * c) for c in range(1, n_chip)]
        prev, stats = None, []
        for g in range(n_chip):
            sib = swap(held[g], 1)
            res = logits_call(
                g, n_chip, vocab_loc, nblk, tokens, dev, held[g], sib, offset.reshape(1), gain32[None, :],
                embed_table if prev is None else e_dev, prev,
            )
            if prev is None:
                e_dev = res[4]
            prev = z, ut, lab = res[:3]
            stats.append(res[3])
        mask_all = jnp.concatenate([st[3] for st in stats]).reshape(n_dp, tokens)
        mask_count = jnp.sum(mask_all)

        stat = jnp.concatenate(stats, axis=1)[:3].reshape(3, n_dp, tokens)
        for axis, mask in (("dp", 1), ("dp", 2), ("dp", 4), ("tp", 1)):
            got = swap(stat, mask, axis)
            if axis == "dp":
                got = jnp.stack([got[:, r ^ mask] for r in range(n_dp)], axis=1)
            top = jnp.maximum(stat[0], got[0])
            stat = jnp.stack([
                top,
                stat[1] * jnp.exp(stat[0] - top) + got[1] * jnp.exp(got[0] - top),
                stat[2] + got[2],
            ])
        log_norm = stat[0] + jnp.log(stat[1])
        wide = lambda a: jnp.broadcast_to(a.reshape(-1)[:, None], (n_dp * tokens, 128))
        lse, wgt = wide(log_norm), wide(mask_all / mask_count)

        def after(x, *deps):
            return lax.optimization_barrier((x, *deps))[0]

        off, out, sent, turn = 0, None, [], dev
        for c, steps in enumerate(CHUNKS):
            pieces = embed_grad(turn, z, lse, wgt, lab, ut, off, steps, n_dp)
            sent.append((off, steps, [pieces[0]] + [swap(pieces[r], r) for r in range(1, n_dp)]))
            turn = after(dev, pieces[0])
            off += steps
            if c == 1:
                odd, = hidden_grad(turn, z, lse, wgt, lab, e_dev, 1, n_dp)
                turn = after(dev, odd)
                got = swap(odd, 1)
            if c == 2:
                even = hidden_grad(turn, z, lse, wgt, lab, e_dev, 0, n_dp, got)
                turn = after(dev, even[0])
        part = even[0]
        for c in range(1, n_chip):
            part = part + swap(even[c], 2 * c)
        grad_norm = part + swap(part, 1, "tp")
        for off, steps, pieces in sent:
            out = place(turn, pieces, out, off, steps, vocab_loc, nblk)
            turn = dev

        inv_rms = lax.rsqrt(jnp.mean(x_full * x_full, axis=-1, keepdims=True) + EPSILON)
        x_hat = x_full * inv_rms
        own = mask_all[0] * (log_norm[0] - stat[2, 0]) * (1.0 / n_tp)
        sums = lax.psum(jnp.concatenate([jnp.sum(grad_norm * x_hat, axis=0) * (1.0 / n_tp), jnp.sum(own)[None]]), ("tp", "dp"))
        grad_gain, loss_value = sums[:hid], sums[hid] / mask_count
        a = grad_norm * gain32
        grad_hidden = inv_rms * (a - x_hat * jnp.mean(a * x_hat, axis=-1, keepdims=True))
        return loss_value, grad_hidden.reshape(n_seq, seq_len, hid), out.T, grad_gain

    return jax.shard_map(
        local_step,
        mesh=mesh,
        in_specs=(P("dp", None, None), P("dp", None), P("dp", None), P(), P("tp", None)),
        out_specs=(P(), P("dp", None, None), P("tp", "dp"), P()),
        check_vma=False,
    )
```

```python
import functools

import jax
import jax.numpy as jnp
from jax import lax
from jax.experimental import pallas as pl
from jax.experimental.pallas import tpu as pltpu
from jax.sharding import PartitionSpec as P


EPSILON = 1e-6
NEG = -1e30
VB = 256
NT = (((1,), (1,)), ((), ()))

CHUNKS = ((0, 3), (3, 7), (15, 4), (10, 5))


def logit_kernel(vocab_loc, nblk, first, d_ref, *refs):
    pieces, (off_ref, gain_ref, e_ref), rest = refs[:2], refs[2:5], refs[5:]
    if first:
        z_ref, ut_ref, lab_ref, st_ref, eo_ref, u_s, m_s, s_s, t_s, l_s = rest
    else:
        _, _, _, z_ref, ut_ref, lab_ref, st_ref, u_s, m_s, s_s, t_s, l_s = rest
    j = pl.program_id(0)
    steps, width = nblk // 2, 2 * VB
    half = u_s.shape[0] // 2
    base = (d_ref[0] * nblk + 2 * j) * VB

    @pl.when(j == 0)
    def _():
        for part, h_ref in enumerate(pieces):
            for i in range(half // 256):
                x = h_ref[i * 256:(i + 1) * 256, :]
                r = lax.rsqrt(jnp.mean(x * x, axis=-1, keepdims=True) + EPSILON)
                y = ((x * r) * gain_ref[...]).astype(jnp.bfloat16)
                at = part * half + i * 256
                u_s[at:at + 256, :] = y
                ut_ref[:, at:at + 256] = y.T
            row = h_ref[half:half + 8, :][:1, :half].astype(jnp.int32) - off_ref[0]
            row = jnp.where(row < vocab_loc, row, -1)
            lab_ref[part * half:(part + 1) * half, :] = jnp.broadcast_to(row, (128, half)).T
        m_s[...] = jnp.full(m_s.shape, NEG, jnp.float32)
        s_s[...] = jnp.zeros(s_s.shape, jnp.float32)
        t_s[...] = jnp.zeros(t_s.shape, jnp.float32)
        l_s[...] = lab_ref[...] - lax.broadcasted_iota(jnp.int32, lab_ref.shape, 1)

    if first:
        rows = lax.broadcasted_iota(jnp.int32, e_ref.shape, 0) + base
        eo_ref[...] = jnp.where(rows < vocab_loc, e_ref[...].astype(jnp.float32), 0.0).astype(jnp.bfloat16)
        e_ref = eo_ref
    bias = jnp.where(lax.broadcasted_iota(jnp.int32, (1, width), 1) + base < vocab_loc, 0.0, NEG)
    for i in range(2 * half // 256):
        sl = slice(i * 256, (i + 1) * 256)
        z = lax.dot_general(u_s[sl, :], e_ref[...], NT, preferred_element_type=jnp.float32) + bias
        z_ref[0, sl, :] = z[:, :VB]
        z_ref[1, sl, :] = z[:, VB:]
        parts = [z[:, k:k + 128] for k in range(0, width, 128)]
        m_old = m_s[sl, :]
        m_new = functools.reduce(jnp.maximum, parts, m_old)
        m_s[sl, :] = m_new
        s_s[sl, :] = s_s[sl, :] * jnp.exp(m_old - m_new) + sum(jnp.exp(p - m_new) for p in parts)
        lab, target = l_s[sl, :], t_s[sl, :]
        for k, p in enumerate(parts):
            target = jnp.where(lab == base + k * 128, p, target)
        t_s[sl, :] = target

    @pl.when(j == steps - 1)
    def _():
        m_all = jnp.max(m_s[...], axis=-1, keepdims=True)
        s_all = jnp.sum(s_s[...] * jnp.exp(m_s[...] - m_all), axis=-1, keepdims=True)
        t_all = jnp.sum(t_s[...], axis=-1, keepdims=True)
        lane = lax.broadcasted_iota(jnp.int32, m_s.shape, 1)
        st_ref[...] = jnp.where(lane == 0, m_all, jnp.where(lane == 1, s_all, t_all)).T[:8, :]
        for part, h_ref in enumerate(pieces):
            st_ref[3:4, part * half:(part + 1) * half] = h_ref[half:half + 8, :][1:2, :half]


def logits_call(group, n_group, vocab_loc, nblk, half, dev, ha, hb, off, gain, embed, prev):
    ext, hid = ha.shape
    tg, width, steps = 2 * half, 2 * VB, nblk // 2
    first = prev is None
    last = (vocab_loc + width - 1) // width - 1
    one = pl.Buffered(1)
    if first:
        e_map = lambda j, d: (jnp.minimum(d[0] * steps + j, last), 0)
    else:
        e_map = lambda j, d: (j, 0)
    in_specs = [
        pl.BlockSpec((ext, hid), lambda j, d: (0, 0), pipeline_mode=one),
        pl.BlockSpec((ext, hid), lambda j, d: (0, 0), pipeline_mode=one),
        pl.BlockSpec(memory_space=pltpu.SMEM),
        pl.BlockSpec((1, hid), lambda j, d: (0, 0)),
        pl.BlockSpec((width, hid), e_map),
    ]
    out_specs = [
        pl.BlockSpec((2, tg, VB), lambda j, d: (j, group, 0)),
        pl.BlockSpec((hid, tg), lambda j, d: (0, group)),
        pl.BlockSpec((tg, 128), lambda j, d: (group, 0)),
        pl.BlockSpec((8, tg), lambda j, d: (0, 0)),
    ]
    out_shape = [
        jax.ShapeDtypeStruct((nblk, n_group * tg, VB), jnp.float32),
        jax.ShapeDtypeStruct((hid, n_group * tg), jnp.bfloat16),
        jax.ShapeDtypeStruct((n_group * tg, 128), jnp.int32),
        jax.ShapeDtypeStruct((8, tg), jnp.float32),
    ]
    args = [dev, ha, hb, off, gain, embed]
    alias = {}
    if first:
        out_specs.append(pl.BlockSpec((width, hid), lambda j, d: (j, 0)))
        out_shape.append(jax.ShapeDtypeStruct((nblk * VB, hid), jnp.bfloat16))
    else:
        in_specs += [pl.BlockSpec(memory_space=pl.ANY)] * 3
        alias = {6: 0, 7: 1, 8: 2}
        args += list(prev)
    return pl.pallas_call(
        functools.partial(logit_kernel, vocab_loc, nblk, first),
        grid_spec=pltpu.PrefetchScalarGridSpec(
            num_scalar_prefetch=1,
            grid=(steps,),
            in_specs=in_specs,
            out_specs=out_specs,
            scratch_shapes=[
                pltpu.VMEM((tg, hid), jnp.bfloat16),
                pltpu.VMEM((tg, 128), jnp.float32),
                pltpu.VMEM((tg, 128), jnp.float32),
                pltpu.VMEM((tg, 128), jnp.float32),
                pltpu.VMEM((tg, 128), jnp.int32),
            ],
        ),
        out_shape=out_shape,
        input_output_aliases=alias,
        compiler_params=pltpu.CompilerParams(vmem_limit_bytes=60 << 20),
        cost_estimate=pl.CostEstimate(flops=2 * tg * nblk * VB * hid, bytes_accessed=4 * tg * nblk * VB, transcendentals=0),
        name="logits",
    )(*args)


def grad_block(z, lse, wgt, lab, base):
    parts = []
    for k in range(VB // 128):
        p = jnp.exp(z[:, k * 128:(k + 1) * 128] - lse)
        p = jnp.where(lab == base + k * 128, p - 1.0, p)
        parts.append((p * wgt).astype(jnp.bfloat16))
    return jnp.concatenate(parts, axis=1)


def hidden_grad_kernel(nblk, inner, n_out, d_ref, z_ref, lse_ref, w_ref, lab_ref, e_ref, *rest):
    lse, wgt = lse_ref[...], w_ref[...]
    lab = lab_ref[...] - lax.broadcasted_iota(jnp.int32, lab_ref.shape, 1)
    acc_s, outs = rest[-1], rest[-1 - n_out:-1]
    acc_s[...] = rest[0][...] if len(rest) > n_out + 1 else jnp.zeros(acc_s.shape, jnp.float32)

    def step(it, carry):
        acc = None
        for k in range(inner):
            j = it * inner + k
            g = grad_block(z_ref[j], lse, wgt, lab, (d_ref[0] * nblk + j) * VB)
            e = e_ref[pl.ds(pl.multiple_of(j * VB, VB), VB), :]
            part = jnp.dot(g, e, preferred_element_type=jnp.float32)
            acc = part if acc is None else acc + part
        acc_s[...] += acc
        return carry

    lax.fori_loop(0, nblk // inner, step, 0)
    if n_out == 1:
        outs[0][...] = acc_s[...]
    else:
        per = pl.num_programs(0) // n_out
        for c in range(n_out):
            @pl.when(pl.program_id(0) // per == c)
            def _():
                outs[c][...] = acc_s[...]


def hidden_grad(dev, z, lse, wgt, lab, e_dev, tb, at, steps, n_out, add=None, add_at=None):
    nblk, _, _ = z.shape
    hid = e_dev.shape[1]
    per = steps // n_out
    wide = pl.BlockSpec((tb, 128), lambda i, d: (at(i, d), 0))
    in_specs = [
        pl.BlockSpec((nblk, tb, VB), lambda i, d: (0, at(i, d), 0)),
        wide, wide, wide,
        pl.BlockSpec((nblk * VB, hid), lambda i, d: (0, 0), pipeline_mode=pl.Buffered(1)),
    ]
    args = [dev, z, lse, wgt, lab, e_dev]
    if add is not None:
        in_specs.append(pl.BlockSpec((tb, hid), lambda i, d: (add_at(i, d), 0)))
        args.append(add)
    out_specs = [
        pl.BlockSpec((tb, hid), functools.partial(lambda c, i, d: (jnp.clip(i - c * per, 0, per - 1), 0), c))
        for c in range(n_out)
    ]
    return pl.pallas_call(
        functools.partial(hidden_grad_kernel, nblk, 19, n_out),
        grid_spec=pltpu.PrefetchScalarGridSpec(
            num_scalar_prefetch=1,
            grid=(steps,),
            in_specs=in_specs,
            out_specs=out_specs,
            scratch_shapes=[pltpu.VMEM((tb, hid), jnp.float32)],
        ),
        out_shape=[jax.ShapeDtypeStruct((per * tb, hid), jnp.float32)] * n_out,
        compiler_params=pltpu.CompilerParams(vmem_limit_bytes=60 << 20),
        cost_estimate=pl.CostEstimate(flops=2 * steps * tb * nblk * VB * hid, bytes_accessed=4 * steps * tb * nblk * VB, transcendentals=0),
        name="hidden_grad",
    )(*args)


def embed_grad_kernel(nblk, off, n_dp, d_ref, z_ref, lse_ref, w_ref, lab_ref, ut_ref, *rest):
    outs, acc_s = rest[:n_dp], rest[n_dp]
    j = pl.program_id(0)
    hid, tokens = ut_ref.shape
    cols = hid // n_dp
    lane = lax.broadcasted_iota(jnp.int32, (256, 128), 1)
    group = tokens // 4
    acc_s[...] = jnp.zeros(acc_s.shape, jnp.float32)

    def step(it, carry):
        acc = None
        for i in range(group // 256):
            sl = pl.ds(pl.multiple_of(it * group + i * 256, 256), 256)
            lse, wgt, lab = lse_ref[sl, :], w_ref[sl, :], lab_ref[sl, :] - lane
            g = jnp.concatenate(
                [grad_block(z_ref[k, sl, :], lse, wgt, lab, (d_ref[0] * nblk + (off + j) * 2 + k) * VB) for k in range(2)],
                axis=1,
            )
            part = jnp.dot(ut_ref[:, sl], g, preferred_element_type=jnp.float32)
            acc = part if acc is None else acc + part
        acc_s[...] += acc
        return carry

    lax.fori_loop(0, 4, step, 0)
    for r in range(n_dp):
        at = pl.multiple_of((d_ref[0] ^ r) * cols, 8)
        outs[r][...] = acc_s[pl.ds(at, cols), :]


def embed_grad(dev, z, lse, wgt, lab, ut, off, steps, n_dp):
    nblk, tokens, _ = z.shape
    hid = ut.shape[0]
    cols = hid // n_dp
    one = pl.Buffered(1)
    wide = pl.BlockSpec((tokens, 128), lambda j, d: (0, 0), pipeline_mode=one)
    return pl.pallas_call(
        functools.partial(embed_grad_kernel, nblk, off, n_dp),
        grid_spec=pltpu.PrefetchScalarGridSpec(
            num_scalar_prefetch=1,
            grid=(steps,),
            in_specs=[
                pl.BlockSpec((2, tokens, VB), lambda j, d: (off + j, 0, 0)),
                wide, wide, wide,
                pl.BlockSpec((hid, tokens), lambda j, d: (0, 0), pipeline_mode=one),
            ],
            out_specs=[pl.BlockSpec((cols, 2 * VB), lambda j, d: (0, j))] * n_dp,
            scratch_shapes=[pltpu.VMEM((hid, 2 * VB), jnp.float32)],
        ),
        out_shape=[jax.ShapeDtypeStruct((cols, steps * 2 * VB), jnp.float32)] * n_dp,
        compiler_params=pltpu.CompilerParams(vmem_limit_bytes=60 << 20),
        cost_estimate=pl.CostEstimate(flops=2 * tokens * steps * 2 * VB * hid, bytes_accessed=8 * tokens * steps * VB, transcendentals=0),
        name="embed_grad",
    )(dev, z, lse, wgt, lab, ut)


def place_copy_kernel(n_dp, per, off, d_ref, *refs):
    pieces, out, (buf, in_sem, out_sem) = refs[:n_dp], refs[-4], refs[-3:]
    width = pieces[0].shape[1]
    loads = [pltpu.make_async_copy(pieces[r], buf.at[r], in_sem.at[r]) for r in range(n_dp)]
    stores = []
    for r in range(n_dp):
        at = pl.multiple_of(((d_ref[0] ^ r) * per + off) * 2 * VB, 2 * VB)
        stores.append(pltpu.make_async_copy(buf.at[r], out.at[:, pl.ds(at, width)], out_sem.at[r]))
    for load in loads:
        load.start()
    for load, store in zip(loads, stores):
        load.wait()
        store.start()
    for store in stores:
        store.wait()


def place_copy(dev, pieces, prev, off, steps, vocab_loc, nblk):
    n_dp, cols = len(pieces), pieces[0].shape[0]
    width = steps * 2 * VB
    anywhere = pl.BlockSpec(memory_space=pl.ANY)
    args = [dev, *pieces]
    alias = {}
    if prev is not None:
        args.append(prev)
        alias = {n_dp + 1: 0}
    return pl.pallas_call(
        functools.partial(place_copy_kernel, n_dp, nblk // 2, off),
        grid_spec=pltpu.PrefetchScalarGridSpec(
            num_scalar_prefetch=1,
            grid=(1,),
            in_specs=[anywhere] * (len(args) - 1),
            out_specs=anywhere,
            scratch_shapes=[
                pltpu.VMEM((n_dp, cols, width), jnp.float32),
                pltpu.SemaphoreType.DMA((n_dp,)),
                pltpu.SemaphoreType.DMA((n_dp,)),
            ],
        ),
        out_shape=jax.ShapeDtypeStruct((cols, vocab_loc), jnp.float32),
        input_output_aliases=alias,
        compiler_params=pltpu.CompilerParams(vmem_limit_bytes=40 << 20),
        cost_estimate=pl.CostEstimate(flops=n_dp * width * cols, bytes_accessed=8 * n_dp * width * cols, transcendentals=0),
    )(*args)


def place_kernel(n_dp, per, off, last, d_ref, *refs):
    pieces, out = refs[:n_dp], refs[-1]
    s, j = pl.program_id(0), pl.program_id(1)
    for r in range(n_dp):
        @pl.when(((s ^ d_ref[0]) == r) & (s * per + off + j <= last))
        def _():
            out[...] = pieces[r][...]


def place(dev, pieces, prev, off, steps, vocab_loc, nblk):
    n_dp, cols = len(pieces), pieces[0].shape[0]
    rows, per = 2 * VB, nblk // 2
    last = (vocab_loc + rows - 1) // rows - 1
    specs = [
        pl.BlockSpec((cols, rows), functools.partial(lambda r, s, j, d: (0, jnp.where((s ^ d[0]) == r, j, 0)), r))
        for r in range(n_dp)
    ]
    args = [dev, *pieces]
    alias = {}
    if prev is not None:
        specs.append(pl.BlockSpec(memory_space=pl.ANY))
        args.append(prev)
        alias = {n_dp + 1: 0}
    return pl.pallas_call(
        functools.partial(place_kernel, n_dp, per, off, last),
        grid_spec=pltpu.PrefetchScalarGridSpec(
            num_scalar_prefetch=1,
            grid=(n_dp, steps),
            in_specs=specs,
            out_specs=pl.BlockSpec((cols, rows), lambda s, j, d: (0, jnp.minimum(s * per + off + j, last))),
        ),
        out_shape=jax.ShapeDtypeStruct((cols, vocab_loc), jnp.float32),
        input_output_aliases=alias,
        cost_estimate=pl.CostEstimate(flops=n_dp * steps * rows * cols, bytes_accessed=8 * n_dp * steps * rows * cols, transcendentals=0),
        name="place",
    )(*args)


def solution(mesh):
    n_dp, n_tp = mesh.shape["dp"], mesh.shape["tp"]

    def swap(x, mask, axis="dp"):
        size = n_dp if axis == "dp" else n_tp
        return lax.ppermute(x, axis, [(i, i ^ mask) for i in range(size)])

    def local_step(hidden, labels, loss_mask, norm_gain, embed_table):
        n_seq, seq_len, hid = hidden.shape
        vocab_loc = embed_table.shape[0]
        tokens = n_seq * seq_len
        unit = 2 * VB * n_dp
        nblk = (vocab_loc + unit - 1) // unit * 2
        me = lax.axis_index("dp").astype(jnp.int32)
        plane = lax.axis_index("tp").astype(jnp.int32)
        dev = jnp.stack([me, plane])
        offset = plane * vocab_loc
        n_chip = n_dp // 2

        x_full = hidden.reshape(tokens, hid).astype(jnp.float32)
        gain32 = norm_gain.astype(jnp.float32)
        ints = jnp.stack([labels.reshape(tokens), loss_mask.reshape(tokens)]).astype(jnp.float32)
        mine = jnp.concatenate([x_full, jnp.pad(ints, ((0, 6), (0, hid - tokens)))])
        held = [mine] + [swap(mine, 2 * c) for c in range(1, n_chip)]
        prev, stats = None, []
        for g in range(n_chip):
            sib = swap(held[g], 1)
            res = logits_call(
                g, n_chip, vocab_loc, nblk, tokens, dev, held[g], sib, offset.reshape(1), gain32[None, :],
                embed_table if prev is None else e_dev, prev,
            )
            if prev is None:
                e_dev = res[4]
            prev = z, ut, lab = res[:3]
            stats.append(res[3])
        mask_all = jnp.concatenate([st[3] for st in stats]).reshape(n_dp, tokens)
        mask_count = jnp.sum(mask_all)

        stat = jnp.concatenate(stats, axis=1)[:3].reshape(3, n_dp, tokens)
        for axis, mask in (("dp", 1), ("dp", 2), ("dp", 4), ("tp", 1)):
            got = swap(stat, mask, axis)
            if axis == "dp":
                got = jnp.stack([got[:, r ^ mask] for r in range(n_dp)], axis=1)
            top = jnp.maximum(stat[0], got[0])
            stat = jnp.stack([
                top,
                stat[1] * jnp.exp(stat[0] - top) + got[1] * jnp.exp(got[0] - top),
                stat[2] + got[2],
            ])
        log_norm = stat[0] + jnp.log(stat[1])
        wide = lambda a: jnp.broadcast_to(a.reshape(-1)[:, None], (n_dp * tokens, 128))
        lse, wgt = wide(log_norm), wide(mask_all / mask_count)

        def after(x, *deps):
            return lax.optimization_barrier((x, *deps))[0]

        half = tokens // 2
        tb = half // 2
        odd_at = lambda i, d: (2 * (i // 3) + 1) * 3 + i % 3
        send_at = lambda i, d: (i // 2) * 8 + (1 - d[1]) * 2 + i % 2
        send_add = lambda i, d: (i // 2) * 4 + (1 - d[1]) * 2 + i % 2
        keep_at = lambda i, d: (i // 2) * 8 + d[1] * 2 + i % 2
        keep_add = lambda i, d: (i // 2) * 4 + d[1] * 2 + i % 2
        sent, turn = [], dev
        for c, (off, steps) in enumerate(CHUNKS):
            if c == len(CHUNKS) - 2:
                odd, = hidden_grad(turn, z, lse, wgt, lab, e_dev, 256, odd_at, 12, 1)
                turn = after(dev, odd)
                got = swap(odd, 1)
            if c == len(CHUNKS) - 1:
                away = hidden_grad(turn, z, lse, wgt, lab, e_dev, tb, send_at, 8, n_chip, got, send_add)
                turn = after(dev, away[0])
                back = [swap(p, 1, "tp") for p in away]
                kept = hidden_grad(turn, z, lse, wgt, lab, e_dev, tb, keep_at, 8, n_chip, got, keep_add)
                turn = after(dev, kept[0])
            pieces = embed_grad(turn, z, lse, wgt, lab, ut, off, steps, n_dp)
            sent.append((off, steps, [pieces[0]] + [swap(pieces[r], r) for r in range(1, n_dp)]))
            turn = after(dev, pieces[0])
        both = [k + b for k, b in zip(kept, back)]
        grad_norm = both[0]
        for c in range(1, n_chip):
            grad_norm = grad_norm + swap(both[c], 2 * c)

        x_half = lax.dynamic_slice_in_dim(hidden.reshape(tokens, hid), plane * half, half).astype(jnp.float32)
        inv_rms = lax.rsqrt(jnp.mean(x_half * x_half, axis=-1, keepdims=True) + EPSILON)
        x_hat = x_half * inv_rms
        a = grad_norm * gain32
        dh_half = inv_rms * (a - x_hat * jnp.mean(a * x_hat, axis=-1, keepdims=True))
        dh_other = swap(dh_half, 1, "tp")
        grad_hidden = jnp.where(plane == 0, jnp.concatenate([dh_half, dh_other]), jnp.concatenate([dh_other, dh_half]))
        own = jnp.sum(mask_all[0] * (log_norm[0] - stat[2, 0])) * (1.0 / n_tp)
        sums = jnp.concatenate([jnp.sum(grad_norm * x_hat, axis=0), own[None]])[None]
        for axis, mask in (("tp", 1), ("dp", 1), ("dp", 2), ("dp", 4)):
            sums = sums + swap(sums, mask, axis)

        out = None
        for c, (off, steps, pieces) in enumerate(sent):
            ragged = n_dp * nblk * VB - (nblk // 2 - off - steps) * 2 * VB > vocab_loc
            turn = dev if c < len(sent) - 1 else after(dev, grad_hidden, sums)
            out = (place if ragged else place_copy)(turn, pieces, out, off, steps, vocab_loc, nblk)

        grad_gain, loss_value = sums[0, :hid], sums[0, hid] / mask_count
        return loss_value, grad_hidden.reshape(n_seq, seq_len, hid), out.T, grad_gain

    return jax.shard_map(
        local_step,
        mesh=mesh,
        in_specs=(P("dp", None, None), P("dp", None), P("dp", None), P(), P("tp", None)),
        out_specs=(P(), P("dp", None, None), P("tp", "dp"), P()),
        check_vma=False,
    )
```

```python
import functools

import jax
import jax.numpy as jnp
from jax import lax
from jax.experimental import pallas as pl
from jax.experimental.pallas import tpu as pltpu
from jax.sharding import PartitionSpec as P


EPSILON = 1e-6
NEG = -1e30
VB = 256
NT = (((1,), (1,)), ((), ()))

CHUNKS = ((0, 4), (4, 7), (13, 6), (11, 2))


def logit_kernel(vocab_loc, nblk, first, d_ref, *refs):
    pieces, (off_ref, gain_ref, e_ref), rest = refs[:2], refs[2:5], refs[5:]
    if first:
        z_ref, ut_ref, lab_ref, st_ref, eo_ref, u_s, m_s, s_s, t_s, l_s = rest
    else:
        _, _, _, z_ref, ut_ref, lab_ref, st_ref, u_s, m_s, s_s, t_s, l_s = rest
    j = pl.program_id(0)
    steps, width = nblk // 2, 2 * VB
    half = u_s.shape[0] // 2
    base = (d_ref[0] * nblk + 2 * j) * VB

    @pl.when(j == 0)
    def _():
        for part, h_ref in enumerate(pieces):
            for i in range(half // 256):
                x = h_ref[i * 256:(i + 1) * 256, :]
                r = lax.rsqrt(jnp.mean(x * x, axis=-1, keepdims=True) + EPSILON)
                y = ((x * r) * gain_ref[...]).astype(jnp.bfloat16)
                at = part * half + i * 256
                u_s[at:at + 256, :] = y
                ut_ref[:, at:at + 256] = y.T
            row = h_ref[half:half + 8, :][:1, :half].astype(jnp.int32) - off_ref[0]
            row = jnp.where(row < vocab_loc, row, -1)
            lab_ref[part * half:(part + 1) * half, :] = jnp.broadcast_to(row, (128, half)).T
        m_s[...] = jnp.full(m_s.shape, NEG, jnp.float32)
        s_s[...] = jnp.zeros(s_s.shape, jnp.float32)
        t_s[...] = jnp.zeros(t_s.shape, jnp.float32)
        l_s[...] = lab_ref[...] - lax.broadcasted_iota(jnp.int32, lab_ref.shape, 1)

    if first:
        rows = lax.broadcasted_iota(jnp.int32, e_ref.shape, 0) + base
        eo_ref[...] = jnp.where(rows < vocab_loc, e_ref[...].astype(jnp.float32), 0.0).astype(jnp.bfloat16)
        e_ref = eo_ref
    bias = jnp.where(lax.broadcasted_iota(jnp.int32, (1, width), 1) + base < vocab_loc, 0.0, NEG)
    for i in range(2 * half // 256):
        sl = slice(i * 256, (i + 1) * 256)
        z = lax.dot_general(u_s[sl, :], e_ref[...], NT, preferred_element_type=jnp.float32) + bias
        z_ref[0, sl, :] = z[:, :VB]
        z_ref[1, sl, :] = z[:, VB:]
        parts = [z[:, k:k + 128] for k in range(0, width, 128)]
        m_old = m_s[sl, :]
        m_new = functools.reduce(jnp.maximum, parts, m_old)
        m_s[sl, :] = m_new
        s_s[sl, :] = s_s[sl, :] * jnp.exp(m_old - m_new) + sum(jnp.exp(p - m_new) for p in parts)
        lab, target = l_s[sl, :], t_s[sl, :]
        for k, p in enumerate(parts):
            target = jnp.where(lab == base + k * 128, p, target)
        t_s[sl, :] = target

    @pl.when(j == steps - 1)
    def _():
        m_all = jnp.max(m_s[...], axis=-1, keepdims=True)
        s_all = jnp.sum(s_s[...] * jnp.exp(m_s[...] - m_all), axis=-1, keepdims=True)
        t_all = jnp.sum(t_s[...], axis=-1, keepdims=True)
        lane = lax.broadcasted_iota(jnp.int32, m_s.shape, 1)
        st_ref[...] = jnp.where(lane == 0, m_all, jnp.where(lane == 1, s_all, t_all)).T[:8, :]
        for part, h_ref in enumerate(pieces):
            st_ref[3:4, part * half:(part + 1) * half] = h_ref[half:half + 8, :][1:2, :half]


def logits_call(group, n_group, vocab_loc, nblk, half, dev, ha, hb, off, gain, embed, prev):
    ext, hid = ha.shape
    tg, width, steps = 2 * half, 2 * VB, nblk // 2
    first = prev is None
    last = (vocab_loc + width - 1) // width - 1
    one = pl.Buffered(1)
    if first:
        e_map = lambda j, d: (jnp.minimum(d[0] * steps + j, last), 0)
    else:
        e_map = lambda j, d: (j, 0)
    in_specs = [
        pl.BlockSpec((ext, hid), lambda j, d: (0, 0), pipeline_mode=one),
        pl.BlockSpec((ext, hid), lambda j, d: (0, 0), pipeline_mode=one),
        pl.BlockSpec(memory_space=pltpu.SMEM),
        pl.BlockSpec((1, hid), lambda j, d: (0, 0)),
        pl.BlockSpec((width, hid), e_map),
    ]
    out_specs = [
        pl.BlockSpec((2, tg, VB), lambda j, d: (j, group, 0)),
        pl.BlockSpec((hid, tg), lambda j, d: (0, group)),
        pl.BlockSpec((tg, 128), lambda j, d: (group, 0)),
        pl.BlockSpec((8, tg), lambda j, d: (0, 0)),
    ]
    out_shape = [
        jax.ShapeDtypeStruct((nblk, n_group * tg, VB), jnp.float32),
        jax.ShapeDtypeStruct((hid, n_group * tg), jnp.bfloat16),
        jax.ShapeDtypeStruct((n_group * tg, 128), jnp.int32),
        jax.ShapeDtypeStruct((8, tg), jnp.float32),
    ]
    args = [dev, ha, hb, off, gain, embed]
    alias = {}
    if first:
        out_specs.append(pl.BlockSpec((width, hid), lambda j, d: (j, 0)))
        out_shape.append(jax.ShapeDtypeStruct((nblk * VB, hid), jnp.bfloat16))
    else:
        in_specs += [pl.BlockSpec(memory_space=pl.ANY)] * 3
        alias = {6: 0, 7: 1, 8: 2}
        args += list(prev)
    return pl.pallas_call(
        functools.partial(logit_kernel, vocab_loc, nblk, first),
        grid_spec=pltpu.PrefetchScalarGridSpec(
            num_scalar_prefetch=1,
            grid=(steps,),
            in_specs=in_specs,
            out_specs=out_specs,
            scratch_shapes=[
                pltpu.VMEM((tg, hid), jnp.bfloat16),
                pltpu.VMEM((tg, 128), jnp.float32),
                pltpu.VMEM((tg, 128), jnp.float32),
                pltpu.VMEM((tg, 128), jnp.float32),
                pltpu.VMEM((tg, 128), jnp.int32),
            ],
        ),
        out_shape=out_shape,
        input_output_aliases=alias,
        compiler_params=pltpu.CompilerParams(vmem_limit_bytes=60 << 20),
        cost_estimate=pl.CostEstimate(flops=2 * tg * nblk * VB * hid, bytes_accessed=4 * tg * nblk * VB, transcendentals=0),
        name="logits",
    )(*args)


def grad_block(z, lse, wgt, lab, base):
    parts = []
    for k in range(VB // 128):
        p = jnp.exp(z[:, k * 128:(k + 1) * 128] - lse)
        p = jnp.where(lab == base + k * 128, p - 1.0, p)
        parts.append((p * wgt).astype(jnp.bfloat16))
    return jnp.concatenate(parts, axis=1)


def hidden_grad_kernel(nblk, inner, n_out, d_ref, z_ref, lse_ref, w_ref, lab_ref, e_hbm, *rest):
    acc_s, e_ref, sem = rest[-3:]
    rest = rest[:-3]
    lse, wgt = lse_ref[...], w_ref[...]
    lab = lab_ref[...] - lax.broadcasted_iota(jnp.int32, lab_ref.shape, 1)
    outs = rest[-n_out:]
    i, it = pl.program_id(0), pl.program_id(1)
    rows = inner * VB

    def copy_of(k):
        sl = pl.ds(pl.multiple_of(k * rows, rows), rows)
        return pltpu.make_async_copy(e_hbm.at[sl, :], e_ref.at[sl, :], sem.at[k])

    @pl.when((i == 0) & (it == 0))
    def _():
        for k in range(nblk // inner):
            copy_of(k).start()

    @pl.when(i == 0)
    def _():
        copy_of(it).wait()

    @pl.when(it == 0)
    def _():
        acc_s[...] = rest[0][...] if len(rest) > n_out else jnp.zeros(acc_s.shape, jnp.float32)

    acc = None
    for k in range(inner):
        j = it * inner + k
        g = grad_block(z_ref[k], lse, wgt, lab, (d_ref[0] * nblk + j) * VB)
        e = e_ref[pl.ds(pl.multiple_of(j * VB, VB), VB), :]
        part = jnp.dot(g, e, preferred_element_type=jnp.float32)
        acc = part if acc is None else acc + part
    acc_s[...] += acc

    per = pl.num_programs(0) // n_out
    for c in range(n_out):
        @pl.when((it == nblk // inner - 1) & (i // per == c))
        def _():
            outs[c][...] = acc_s[...]


def hidden_grad(dev, z, lse, wgt, lab, e_dev, tb, at, steps, n_out, add=None, add_at=None):
    nblk, _, _ = z.shape
    hid = e_dev.shape[1]
    per = steps // n_out
    inner = nblk // 2
    wide = pl.BlockSpec((tb, 128), lambda i, t, d: (at(i, d), 0))
    in_specs = [
        pl.BlockSpec((inner, tb, VB), lambda i, t, d: (t, at(i, d), 0)),
        wide, wide, wide,
        pl.BlockSpec(memory_space=pl.ANY),
    ]
    args = [dev, z, lse, wgt, lab, e_dev]
    if add is not None:
        in_specs.append(pl.BlockSpec((tb, hid), lambda i, t, d: (add_at(i, d), 0)))
        args.append(add)
    out_specs = [
        pl.BlockSpec((tb, hid), functools.partial(lambda c, i, t, d: (jnp.clip(i - c * per, 0, per - 1), 0), c))
        for c in range(n_out)
    ]
    return pl.pallas_call(
        functools.partial(hidden_grad_kernel, nblk, inner, n_out),
        grid_spec=pltpu.PrefetchScalarGridSpec(
            num_scalar_prefetch=1,
            grid=(steps, 2),
            in_specs=in_specs,
            out_specs=out_specs,
            scratch_shapes=[
                pltpu.VMEM((tb, hid), jnp.float32),
                pltpu.VMEM((nblk * VB, hid), jnp.bfloat16),
                pltpu.SemaphoreType.DMA((2,)),
            ],
        ),
        out_shape=[jax.ShapeDtypeStruct((per * tb, hid), jnp.float32)] * n_out,
        compiler_params=pltpu.CompilerParams(vmem_limit_bytes=60 << 20),
        cost_estimate=pl.CostEstimate(flops=2 * steps * tb * nblk * VB * hid, bytes_accessed=4 * steps * tb * nblk * VB, transcendentals=0),
        name="hidden_grad",
    )(*args)


def embed_grad_kernel(nblk, off, n_dp, d_ref, z_ref, *rest):
    hbm, outs, acc_s, held, sem = rest[:4], rest[4:4 + n_dp], rest[4 + n_dp], rest[5 + n_dp:9 + n_dp], rest[9 + n_dp]
    lse_ref, w_ref, lab_ref, ut_ref = held
    j, it = pl.program_id(0), pl.program_id(1)
    hid, tokens = ut_ref.shape
    cols = hid // n_dp
    lane = lax.broadcasted_iota(jnp.int32, (256, 128), 1)
    n_group = tokens // z_ref.shape[1]
    group = tokens // n_group

    def copies(it):
        sl = pl.ds(pl.multiple_of(it * group, group), group)
        for k, (src, dst) in enumerate(zip(hbm, held)):
            at = (slice(None), sl) if k == 3 else (sl, slice(None))
            yield pltpu.make_async_copy(src.at[at], dst.at[at], sem.at[it, k])

    @pl.when((j == 0) & (it == 0))
    def _():
        for g in range(n_group):
            for copy in copies(g):
                copy.start()

    @pl.when(j == 0)
    def _():
        for copy in copies(it):
            copy.wait()

    @pl.when(it == 0)
    def _():
        acc_s[...] = jnp.zeros(acc_s.shape, jnp.float32)

    acc = None
    for i in range(group // 256):
        sl = pl.ds(pl.multiple_of(it * group + i * 256, 256), 256)
        lse, wgt, lab = lse_ref[sl, :], w_ref[sl, :], lab_ref[sl, :] - lane
        g = jnp.concatenate(
            [
                grad_block(z_ref[k, i * 256:(i + 1) * 256, :], lse, wgt, lab, (d_ref[0] * nblk + (off + j) * 2 + k) * VB)
                for k in range(2)
            ],
            axis=1,
        )
        part = jnp.dot(ut_ref[:, sl], g, preferred_element_type=jnp.float32)
        acc = part if acc is None else acc + part
    acc_s[...] += acc

    @pl.when(it == n_group - 1)
    def _():
        for r in range(n_dp):
            at = pl.multiple_of((d_ref[0] ^ r) * cols, 8)
            outs[r][...] = acc_s[pl.ds(at, cols), :]


def embed_grad(dev, z, lse, wgt, lab, ut, off, steps, n_dp):
    nblk, tokens, _ = z.shape
    hid = ut.shape[0]
    cols = hid // n_dp
    return pl.pallas_call(
        functools.partial(embed_grad_kernel, nblk, off, n_dp),
        grid_spec=pltpu.PrefetchScalarGridSpec(
            num_scalar_prefetch=1,
            grid=(steps, 2),
            in_specs=[
                pl.BlockSpec((2, tokens // 2, VB), lambda j, t, d: (off + j, t, 0)),
            ] + [pl.BlockSpec(memory_space=pl.ANY)] * 4,
            out_specs=[pl.BlockSpec((cols, 2 * VB), lambda j, t, d: (0, j))] * n_dp,
            scratch_shapes=[
                pltpu.VMEM((hid, 2 * VB), jnp.float32),
                pltpu.VMEM((tokens, 128), jnp.float32),
                pltpu.VMEM((tokens, 128), jnp.float32),
                pltpu.VMEM((tokens, 128), jnp.int32),
                pltpu.VMEM((hid, tokens), jnp.bfloat16),
                pltpu.SemaphoreType.DMA((2, 4)),
            ],
        ),
        out_shape=[jax.ShapeDtypeStruct((cols, steps * 2 * VB), jnp.float32)] * n_dp,
        compiler_params=pltpu.CompilerParams(vmem_limit_bytes=60 << 20),
        cost_estimate=pl.CostEstimate(flops=2 * tokens * steps * 2 * VB * hid, bytes_accessed=8 * tokens * steps * VB, transcendentals=0),
        name="embed_grad",
    )(dev, z, lse, wgt, lab, ut)


def place_copy_kernel(n_dp, per, off, d_ref, *refs):
    pieces, out, (buf, in_sem, out_sem) = refs[:n_dp], refs[-4], refs[-3:]
    width = pieces[0].shape[1]
    loads = [pltpu.make_async_copy(pieces[r], buf.at[r], in_sem.at[r]) for r in range(n_dp)]
    stores = []
    for r in range(n_dp):
        at = pl.multiple_of(((d_ref[0] ^ r) * per + off) * 2 * VB, 2 * VB)
        stores.append(pltpu.make_async_copy(buf.at[r], out.at[:, pl.ds(at, width)], out_sem.at[r]))
    for load in loads:
        load.start()
    for load, store in zip(loads, stores):
        load.wait()
        store.start()
    for store in stores:
        store.wait()


def place_copy(dev, pieces, prev, off, steps, vocab_loc, nblk):
    n_dp, cols = len(pieces), pieces[0].shape[0]
    width = steps * 2 * VB
    anywhere = pl.BlockSpec(memory_space=pl.ANY)
    args = [dev, *pieces]
    alias = {}
    if prev is not None:
        args.append(prev)
        alias = {n_dp + 1: 0}
    return pl.pallas_call(
        functools.partial(place_copy_kernel, n_dp, nblk // 2, off),
        grid_spec=pltpu.PrefetchScalarGridSpec(
            num_scalar_prefetch=1,
            grid=(1,),
            in_specs=[anywhere] * (len(args) - 1),
            out_specs=anywhere,
            scratch_shapes=[
                pltpu.VMEM((n_dp, cols, width), jnp.float32),
                pltpu.SemaphoreType.DMA((n_dp,)),
                pltpu.SemaphoreType.DMA((n_dp,)),
            ],
        ),
        out_shape=jax.ShapeDtypeStruct((cols, vocab_loc), jnp.float32),
        input_output_aliases=alias,
        compiler_params=pltpu.CompilerParams(vmem_limit_bytes=40 << 20),
        cost_estimate=pl.CostEstimate(flops=n_dp * width * cols, bytes_accessed=8 * n_dp * width * cols, transcendentals=0),
    )(*args)


def place_kernel(n_dp, per, off, last, d_ref, *refs):
    pieces, out = refs[:n_dp], refs[-1]
    s, j = pl.program_id(0), pl.program_id(1)
    for r in range(n_dp):
        @pl.when(((s ^ d_ref[0]) == r) & (s * per + off + j <= last))
        def _():
            out[...] = pieces[r][...]


def place(dev, pieces, prev, off, steps, vocab_loc, nblk):
    n_dp, cols = len(pieces), pieces[0].shape[0]
    rows, per = 2 * VB, nblk // 2
    last = (vocab_loc + rows - 1) // rows - 1
    specs = [
        pl.BlockSpec((cols, rows), functools.partial(lambda r, s, j, d: (0, jnp.where((s ^ d[0]) == r, j, 0)), r))
        for r in range(n_dp)
    ]
    args = [dev, *pieces]
    alias = {}
    if prev is not None:
        specs.append(pl.BlockSpec(memory_space=pl.ANY))
        args.append(prev)
        alias = {n_dp + 1: 0}
    return pl.pallas_call(
        functools.partial(place_kernel, n_dp, per, off, last),
        grid_spec=pltpu.PrefetchScalarGridSpec(
            num_scalar_prefetch=1,
            grid=(n_dp, steps),
            in_specs=specs,
            out_specs=pl.BlockSpec((cols, rows), lambda s, j, d: (0, jnp.minimum(s * per + off + j, last))),
        ),
        out_shape=jax.ShapeDtypeStruct((cols, vocab_loc), jnp.float32),
        input_output_aliases=alias,
        cost_estimate=pl.CostEstimate(flops=n_dp * steps * rows * cols, bytes_accessed=8 * n_dp * steps * rows * cols, transcendentals=0),
        name="place",
    )(*args)


def solution(mesh):
    n_dp, n_tp = mesh.shape["dp"], mesh.shape["tp"]

    def swap(x, mask, axis="dp"):
        size = n_dp if axis == "dp" else n_tp
        return lax.ppermute(x, axis, [(i, i ^ mask) for i in range(size)])

    def local_step(hidden, labels, loss_mask, norm_gain, embed_table):
        n_seq, seq_len, hid = hidden.shape
        vocab_loc = embed_table.shape[0]
        tokens = n_seq * seq_len
        unit = 2 * VB * n_dp
        nblk = (vocab_loc + unit - 1) // unit * 2
        me = lax.axis_index("dp").astype(jnp.int32)
        plane = lax.axis_index("tp").astype(jnp.int32)
        dev = jnp.stack([me, plane])
        offset = plane * vocab_loc
        n_chip = n_dp // 2

        x_full = hidden.reshape(tokens, hid).astype(jnp.float32)
        gain32 = norm_gain.astype(jnp.float32)
        ints = jnp.stack([labels.reshape(tokens), loss_mask.reshape(tokens)]).astype(jnp.float32)
        mine = jnp.concatenate([x_full, jnp.pad(ints, ((0, 6), (0, hid - tokens)))])
        held = [mine] + [swap(mine, 2 * c) for c in range(1, n_chip)]
        prev, stats = None, []
        for g in range(n_chip):
            sib = swap(held[g], 1)
            res = logits_call(
                g, n_chip, vocab_loc, nblk, tokens, dev, held[g], sib, offset.reshape(1), gain32[None, :],
                embed_table if prev is None else e_dev, prev,
            )
            if prev is None:
                e_dev = res[4]
            prev = z, ut, lab = res[:3]
            stats.append(res[3])
        mask_all = jnp.concatenate([st[3] for st in stats]).reshape(n_dp, tokens)
        mask_count = jnp.sum(mask_all)

        stat = jnp.concatenate(stats, axis=1)[:3].reshape(3, n_dp, tokens)
        for axis, mask in (("dp", 1), ("dp", 2), ("dp", 4), ("tp", 1)):
            got = swap(stat, mask, axis)
            if axis == "dp":
                got = jnp.stack([got[:, r ^ mask] for r in range(n_dp)], axis=1)
            top = jnp.maximum(stat[0], got[0])
            stat = jnp.stack([
                top,
                stat[1] * jnp.exp(stat[0] - top) + got[1] * jnp.exp(got[0] - top),
                stat[2] + got[2],
            ])
        log_norm = stat[0] + jnp.log(stat[1])
        wide = lambda a: jnp.broadcast_to(a.reshape(-1)[:, None], (n_dp * tokens, 128))
        lse, wgt = wide(log_norm), wide(mask_all / mask_count)

        def after(x, *deps):
            return lax.optimization_barrier((x, *deps))[0]

        half = tokens // 2
        tb = half // 2
        odd_at = lambda i, d: (2 * (i // 3) + 1) * 3 + i % 3
        send_at = lambda i, d: (i // 2) * 8 + (1 - d[1]) * 2 + i % 2
        send_add = lambda i, d: (i // 2) * 4 + (1 - d[1]) * 2 + i % 2
        keep_at = lambda i, d: (i // 2) * 8 + d[1] * 2 + i % 2
        keep_add = lambda i, d: (i // 2) * 4 + d[1] * 2 + i % 2
        sent, turn = [], dev
        for c, (off, steps) in enumerate(CHUNKS):
            if c == len(CHUNKS) - 2:
                odd, = hidden_grad(turn, z, lse, wgt, lab, e_dev, 256, odd_at, 12, 1)
                turn = after(dev, odd)
                got = swap(odd, 1)
            if c == len(CHUNKS) - 1:
                away = hidden_grad(turn, z, lse, wgt, lab, e_dev, tb, send_at, 8, n_chip, got, send_add)
                turn = after(dev, away[0])
                back = [swap(p, 1, "tp") for p in away]
                kept = hidden_grad(turn, z, lse, wgt, lab, e_dev, tb, keep_at, 8, n_chip, got, keep_add)
                turn = after(dev, kept[0])
            pieces = embed_grad(turn, z, lse, wgt, lab, ut, off, steps, n_dp)
            sent.append((off, steps, [pieces[0]] + [swap(pieces[r], r) for r in range(1, n_dp)]))
            turn = after(dev, pieces[0])
        both = [k + b for k, b in zip(kept, back)]
        grad_norm = both[0]
        for c in range(1, n_chip):
            grad_norm = grad_norm + swap(both[c], 2 * c)

        x_half = lax.dynamic_slice_in_dim(hidden.reshape(tokens, hid), plane * half, half).astype(jnp.float32)
        inv_rms = lax.rsqrt(jnp.mean(x_half * x_half, axis=-1, keepdims=True) + EPSILON)
        x_hat = x_half * inv_rms
        a = grad_norm * gain32
        dh_half = inv_rms * (a - x_hat * jnp.mean(a * x_hat, axis=-1, keepdims=True))
        dh_other = swap(dh_half, 1, "tp")
        grad_hidden = jnp.where(plane == 0, jnp.concatenate([dh_half, dh_other]), jnp.concatenate([dh_other, dh_half]))
        own = jnp.sum(mask_all[0] * (log_norm[0] - stat[2, 0])) * (1.0 / n_tp)
        sums = jnp.concatenate([jnp.sum(grad_norm * x_hat, axis=0), own[None]])[None]
        for axis, mask in (("tp", 1), ("dp", 1), ("dp", 2), ("dp", 4)):
            sums = sums + swap(sums, mask, axis)

        out = None
        for c, (off, steps, pieces) in enumerate(sent):
            ragged = n_dp * nblk * VB - (nblk // 2 - off - steps) * 2 * VB > vocab_loc
            turn = dev if c < len(sent) - 1 else after(dev, grad_hidden, sums)
            out = (place if ragged else place_copy)(turn, pieces, out, off, steps, vocab_loc, nblk)

        grad_gain, loss_value = sums[0, :hid], sums[0, hid] / mask_count
        return loss_value, grad_hidden.reshape(n_seq, seq_len, hid), out.T, grad_gain

    return jax.shard_map(
        local_step,
        mesh=mesh,
        in_specs=(P("dp", None, None), P("dp", None), P("dp", None), P(), P("tp", None)),
        out_specs=(P(), P("dp", None, None), P("tp", "dp"), P()),
        check_vma=False,
    )
```

```python
import functools

import jax
import jax.numpy as jnp
from jax import lax
from jax.experimental import pallas as pl
from jax.experimental.pallas import tpu as pltpu
from jax.sharding import PartitionSpec as P


EPSILON = 1e-6
NEG = -1e30
VB = 256
NT = (((1,), (1,)), ((), ()))

CHUNKS = ((0, 3), (3, 7), (13, 6), (10, 3))


def logit_kernel(vocab_loc, nblk, first, d_ref, *refs):
    pieces, (off_ref, gain_ref, e_ref), rest = refs[:2], refs[2:5], refs[5:]
    if first:
        z_ref, ut_ref, lab_ref, st_ref, eo_ref, u_s, m_s, s_s, t_s, l_s = rest
    else:
        _, _, _, z_ref, ut_ref, lab_ref, st_ref, u_s, m_s, s_s, t_s, l_s = rest
    j = pl.program_id(0)
    steps, width = nblk // 2, 2 * VB
    half = u_s.shape[0] // 2
    base = (d_ref[0] * nblk + 2 * j) * VB

    @pl.when(j == 0)
    def _():
        for part, h_ref in enumerate(pieces):
            for i in range(half // 256):
                x = h_ref[i * 256:(i + 1) * 256, :]
                r = lax.rsqrt(jnp.mean(x * x, axis=-1, keepdims=True) + EPSILON)
                y = ((x * r) * gain_ref[...]).astype(jnp.bfloat16)
                at = part * half + i * 256
                u_s[at:at + 256, :] = y
                ut_ref[:, at:at + 256] = y.T
            row = h_ref[half:half + 8, :][:1, :half].astype(jnp.int32) - off_ref[0]
            row = jnp.where(row < vocab_loc, row, -1)
            lab_ref[part * half:(part + 1) * half, :] = jnp.broadcast_to(row, (128, half)).T
        m_s[...] = jnp.full(m_s.shape, NEG, jnp.float32)
        s_s[...] = jnp.zeros(s_s.shape, jnp.float32)
        t_s[...] = jnp.zeros(t_s.shape, jnp.float32)
        l_s[...] = lab_ref[...] - lax.broadcasted_iota(jnp.int32, lab_ref.shape, 1)

    if first:
        rows = lax.broadcasted_iota(jnp.int32, e_ref.shape, 0) + base
        eo_ref[...] = jnp.where(rows < vocab_loc, e_ref[...].astype(jnp.float32), 0.0).astype(jnp.bfloat16)
        e_ref = eo_ref
    bias = jnp.where(lax.broadcasted_iota(jnp.int32, (1, width), 1) + base < vocab_loc, 0.0, NEG)
    for i in range(2 * half // 256):
        sl = slice(i * 256, (i + 1) * 256)
        z = lax.dot_general(u_s[sl, :], e_ref[...], NT, preferred_element_type=jnp.float32) + bias
        z_ref[0, sl, :] = z[:, :VB]
        z_ref[1, sl, :] = z[:, VB:]
        parts = [z[:, k:k + 128] for k in range(0, width, 128)]
        m_old = m_s[sl, :]
        m_new = functools.reduce(jnp.maximum, parts, m_old)
        m_s[sl, :] = m_new
        s_s[sl, :] = s_s[sl, :] * jnp.exp(m_old - m_new) + sum(jnp.exp(p - m_new) for p in parts)
        lab, target = l_s[sl, :], t_s[sl, :]
        for k, p in enumerate(parts):
            target = jnp.where(lab == base + k * 128, p, target)
        t_s[sl, :] = target

    @pl.when(j == steps - 1)
    def _():
        m_all = jnp.max(m_s[...], axis=-1, keepdims=True)
        s_all = jnp.sum(s_s[...] * jnp.exp(m_s[...] - m_all), axis=-1, keepdims=True)
        t_all = jnp.sum(t_s[...], axis=-1, keepdims=True)
        lane = lax.broadcasted_iota(jnp.int32, m_s.shape, 1)
        st_ref[...] = jnp.where(lane == 0, m_all, jnp.where(lane == 1, s_all, t_all)).T[:8, :]
        for part, h_ref in enumerate(pieces):
            st_ref[3:4, part * half:(part + 1) * half] = h_ref[half:half + 8, :][1:2, :half]


def logits_call(group, n_group, vocab_loc, nblk, half, dev, ha, hb, off, gain, embed, prev):
    ext, hid = ha.shape
    tg, width, steps = 2 * half, 2 * VB, nblk // 2
    first = prev is None
    last = (vocab_loc + width - 1) // width - 1
    one = pl.Buffered(1)
    if first:
        e_map = lambda j, d: (jnp.minimum(d[0] * steps + j, last), 0)
    else:
        e_map = lambda j, d: (j, 0)
    in_specs = [
        pl.BlockSpec((ext, hid), lambda j, d: (0, 0), pipeline_mode=one),
        pl.BlockSpec((ext, hid), lambda j, d: (0, 0), pipeline_mode=one),
        pl.BlockSpec(memory_space=pltpu.SMEM),
        pl.BlockSpec((1, hid), lambda j, d: (0, 0)),
        pl.BlockSpec((width, hid), e_map),
    ]
    out_specs = [
        pl.BlockSpec((2, tg, VB), lambda j, d: (j, group, 0)),
        pl.BlockSpec((hid, tg), lambda j, d: (0, group)),
        pl.BlockSpec((tg, 128), lambda j, d: (group, 0)),
        pl.BlockSpec((8, tg), lambda j, d: (0, 0)),
    ]
    out_shape = [
        jax.ShapeDtypeStruct((nblk, n_group * tg, VB), jnp.float32),
        jax.ShapeDtypeStruct((hid, n_group * tg), jnp.bfloat16),
        jax.ShapeDtypeStruct((n_group * tg, 128), jnp.int32),
        jax.ShapeDtypeStruct((8, tg), jnp.float32),
    ]
    args = [dev, ha, hb, off, gain, embed]
    alias = {}
    if first:
        out_specs.append(pl.BlockSpec((width, hid), lambda j, d: (j, 0)))
        out_shape.append(jax.ShapeDtypeStruct((nblk * VB, hid), jnp.bfloat16))
    else:
        in_specs += [pl.BlockSpec(memory_space=pl.ANY)] * 3
        alias = {6: 0, 7: 1, 8: 2}
        args += list(prev)
    return pl.pallas_call(
        functools.partial(logit_kernel, vocab_loc, nblk, first),
        grid_spec=pltpu.PrefetchScalarGridSpec(
            num_scalar_prefetch=1,
            grid=(steps,),
            in_specs=in_specs,
            out_specs=out_specs,
            scratch_shapes=[
                pltpu.VMEM((tg, hid), jnp.bfloat16),
                pltpu.VMEM((tg, 128), jnp.float32),
                pltpu.VMEM((tg, 128), jnp.float32),
                pltpu.VMEM((tg, 128), jnp.float32),
                pltpu.VMEM((tg, 128), jnp.int32),
            ],
        ),
        out_shape=out_shape,
        input_output_aliases=alias,
        compiler_params=pltpu.CompilerParams(vmem_limit_bytes=60 << 20),
        cost_estimate=pl.CostEstimate(flops=2 * tg * nblk * VB * hid, bytes_accessed=4 * tg * nblk * VB, transcendentals=0),
        name="logits",
    )(*args)


def grad_block(z, lse, wgt, lab, base):
    parts = []
    for k in range(VB // 128):
        p = jnp.exp(z[:, k * 128:(k + 1) * 128] - lse)
        p = jnp.where(lab == base + k * 128, p - 1.0, p)
        parts.append((p * wgt).astype(jnp.bfloat16))
    return jnp.concatenate(parts, axis=1)


def hidden_grad_kernel(nblk, inner, n_out, d_ref, z_ref, lse_ref, w_ref, lab_ref, e_hbm, *rest):
    acc_s, e_ref, sem = rest[-3:]
    rest = rest[:-3]
    lse, wgt = lse_ref[...], w_ref[...]
    lab = lab_ref[...] - lax.broadcasted_iota(jnp.int32, lab_ref.shape, 1)
    outs = rest[-n_out:]
    i, it = pl.program_id(0), pl.program_id(1)
    rows = inner * VB

    def copy_of(k):
        sl = pl.ds(pl.multiple_of(k * rows, rows), rows)
        return pltpu.make_async_copy(e_hbm.at[sl, :], e_ref.at[sl, :], sem.at[k])

    @pl.when((i == 0) & (it == 0))
    def _():
        for k in range(nblk // inner):
            copy_of(k).start()

    @pl.when(i == 0)
    def _():
        copy_of(it).wait()

    @pl.when(it == 0)
    def _():
        acc_s[...] = rest[0][...] if len(rest) > n_out else jnp.zeros(acc_s.shape, jnp.float32)

    acc = None
    for k in range(inner):
        j = it * inner + k
        g = grad_block(z_ref[k], lse, wgt, lab, (d_ref[0] * nblk + j) * VB)
        e = e_ref[pl.ds(pl.multiple_of(j * VB, VB), VB), :]
        part = jnp.dot(g, e, preferred_element_type=jnp.float32)
        acc = part if acc is None else acc + part
    acc_s[...] += acc

    per = pl.num_programs(0) // n_out
    for c in range(n_out):
        @pl.when((it == nblk // inner - 1) & (i // per == c))
        def _():
            outs[c][...] = acc_s[...]


def hidden_grad(dev, z, lse, wgt, lab, e_dev, tb, at, steps, n_out, add=None, add_at=None):
    nblk, _, _ = z.shape
    hid = e_dev.shape[1]
    per = steps // n_out
    inner = nblk // 2
    wide = pl.BlockSpec((tb, 128), lambda i, t, d: (at(i, d), 0))
    in_specs = [
        pl.BlockSpec((inner, tb, VB), lambda i, t, d: (t, at(i, d), 0)),
        wide, wide, wide,
        pl.BlockSpec(memory_space=pl.ANY),
    ]
    args = [dev, z, lse, wgt, lab, e_dev]
    if add is not None:
        in_specs.append(pl.BlockSpec((tb, hid), lambda i, t, d: (add_at(i, d), 0)))
        args.append(add)
    out_specs = [
        pl.BlockSpec((tb, hid), functools.partial(lambda c, i, t, d: (jnp.clip(i - c * per, 0, per - 1), 0), c))
        for c in range(n_out)
    ]
    return pl.pallas_call(
        functools.partial(hidden_grad_kernel, nblk, inner, n_out),
        grid_spec=pltpu.PrefetchScalarGridSpec(
            num_scalar_prefetch=1,
            grid=(steps, 2),
            in_specs=in_specs,
            out_specs=out_specs,
            scratch_shapes=[
                pltpu.VMEM((tb, hid), jnp.float32),
                pltpu.VMEM((nblk * VB, hid), jnp.bfloat16),
                pltpu.SemaphoreType.DMA((2,)),
            ],
        ),
        out_shape=[jax.ShapeDtypeStruct((per * tb, hid), jnp.float32)] * n_out,
        compiler_params=pltpu.CompilerParams(vmem_limit_bytes=60 << 20),
        cost_estimate=pl.CostEstimate(flops=2 * steps * tb * nblk * VB * hid, bytes_accessed=4 * steps * tb * nblk * VB, transcendentals=0),
        name="hidden_grad",
    )(*args)


def embed_grad_kernel(nblk, off, n_dp, d_ref, z_ref, *rest):
    hbm, outs, acc_s, held, sem = rest[:4], rest[4:4 + n_dp], rest[4 + n_dp], rest[5 + n_dp:9 + n_dp], rest[9 + n_dp]
    lse_ref, w_ref, lab_ref, ut_ref = held
    j, it = pl.program_id(0), pl.program_id(1)
    hid, tokens = ut_ref.shape
    cols = hid // n_dp
    lane = lax.broadcasted_iota(jnp.int32, (256, 128), 1)
    n_group = tokens // z_ref.shape[1]
    group = tokens // n_group

    def copies(it):
        sl = pl.ds(pl.multiple_of(it * group, group), group)
        for k, (src, dst) in enumerate(zip(hbm, held)):
            at = (slice(None), sl) if k == 3 else (sl, slice(None))
            yield pltpu.make_async_copy(src.at[at], dst.at[at], sem.at[it, k])

    @pl.when((j == 0) & (it == 0))
    def _():
        for g in range(n_group):
            for copy in copies(g):
                copy.start()

    @pl.when(j == 0)
    def _():
        for copy in copies(it):
            copy.wait()

    @pl.when(it == 0)
    def _():
        acc_s[...] = jnp.zeros(acc_s.shape, jnp.float32)

    acc = None
    for i in range(group // 256):
        sl = pl.ds(pl.multiple_of(it * group + i * 256, 256), 256)
        lse, wgt, lab = lse_ref[sl, :], w_ref[sl, :], lab_ref[sl, :] - lane
        g = jnp.concatenate(
            [
                grad_block(z_ref[k, i * 256:(i + 1) * 256, :], lse, wgt, lab, (d_ref[0] * nblk + (off + j) * 2 + k) * VB)
                for k in range(2)
            ],
            axis=1,
        )
        part = jnp.dot(ut_ref[:, sl], g, preferred_element_type=jnp.float32)
        acc = part if acc is None else acc + part
    acc_s[...] += acc

    @pl.when(it == n_group - 1)
    def _():
        for r in range(n_dp):
            at = pl.multiple_of((d_ref[0] ^ r) * cols, 8)
            outs[r][...] = acc_s[pl.ds(at, cols), :]


def embed_grad(dev, z, lse, wgt, lab, ut, off, steps, n_dp):
    nblk, tokens, _ = z.shape
    hid = ut.shape[0]
    cols = hid // n_dp
    return pl.pallas_call(
        functools.partial(embed_grad_kernel, nblk, off, n_dp),
        grid_spec=pltpu.PrefetchScalarGridSpec(
            num_scalar_prefetch=1,
            grid=(steps, 2),
            in_specs=[
                pl.BlockSpec((2, tokens // 2, VB), lambda j, t, d: (off + j, t, 0)),
            ] + [pl.BlockSpec(memory_space=pl.ANY)] * 4,
            out_specs=[pl.BlockSpec((cols, 2 * VB), lambda j, t, d: (0, j))] * n_dp,
            scratch_shapes=[
                pltpu.VMEM((hid, 2 * VB), jnp.float32),
                pltpu.VMEM((tokens, 128), jnp.float32),
                pltpu.VMEM((tokens, 128), jnp.float32),
                pltpu.VMEM((tokens, 128), jnp.int32),
                pltpu.VMEM((hid, tokens), jnp.bfloat16),
                pltpu.SemaphoreType.DMA((2, 4)),
            ],
        ),
        out_shape=[jax.ShapeDtypeStruct((cols, steps * 2 * VB), jnp.float32)] * n_dp,
        compiler_params=pltpu.CompilerParams(vmem_limit_bytes=60 << 20),
        cost_estimate=pl.CostEstimate(flops=2 * tokens * steps * 2 * VB * hid, bytes_accessed=8 * tokens * steps * VB, transcendentals=0),
        name="embed_grad",
    )(dev, z, lse, wgt, lab, ut)


def place_copy_kernel(n_dp, per, off, d_ref, *refs):
    pieces, out, (buf, in_sem, out_sem) = refs[:n_dp], refs[-4], refs[-3:]
    width = pieces[0].shape[1]
    loads = [pltpu.make_async_copy(pieces[r], buf.at[r], in_sem.at[r]) for r in range(n_dp)]
    stores = []
    for r in range(n_dp):
        at = pl.multiple_of(((d_ref[0] ^ r) * per + off) * 2 * VB, 2 * VB)
        stores.append(pltpu.make_async_copy(buf.at[r], out.at[:, pl.ds(at, width)], out_sem.at[r]))
    for load in loads:
        load.start()
    for load, store in zip(loads, stores):
        load.wait()
        store.start()
    for store in stores:
        store.wait()


def place_copy(dev, pieces, prev, off, steps, vocab_loc, nblk):
    n_dp, cols = len(pieces), pieces[0].shape[0]
    width = steps * 2 * VB
    anywhere = pl.BlockSpec(memory_space=pl.ANY)
    args = [dev, *pieces]
    alias = {}
    if prev is not None:
        args.append(prev)
        alias = {n_dp + 1: 0}
    return pl.pallas_call(
        functools.partial(place_copy_kernel, n_dp, nblk // 2, off),
        grid_spec=pltpu.PrefetchScalarGridSpec(
            num_scalar_prefetch=1,
            grid=(1,),
            in_specs=[anywhere] * (len(args) - 1),
            out_specs=anywhere,
            scratch_shapes=[
                pltpu.VMEM((n_dp, cols, width), jnp.float32),
                pltpu.SemaphoreType.DMA((n_dp,)),
                pltpu.SemaphoreType.DMA((n_dp,)),
            ],
        ),
        out_shape=jax.ShapeDtypeStruct((cols, vocab_loc), jnp.float32),
        input_output_aliases=alias,
        compiler_params=pltpu.CompilerParams(vmem_limit_bytes=40 << 20),
        cost_estimate=pl.CostEstimate(flops=n_dp * width * cols, bytes_accessed=8 * n_dp * width * cols, transcendentals=0),
    )(*args)


def place_kernel(n_dp, per, off, last, d_ref, *refs):
    pieces, out = refs[:n_dp], refs[-1]
    s, j = pl.program_id(0), pl.program_id(1)
    for r in range(n_dp):
        @pl.when(((s ^ d_ref[0]) == r) & (s * per + off + j <= last))
        def _():
            out[...] = pieces[r][...]


def place(dev, pieces, prev, off, steps, vocab_loc, nblk):
    n_dp, cols = len(pieces), pieces[0].shape[0]
    rows, per = 2 * VB, nblk // 2
    last = (vocab_loc + rows - 1) // rows - 1
    specs = [
        pl.BlockSpec((cols, rows), functools.partial(lambda r, s, j, d: (0, jnp.where((s ^ d[0]) == r, j, 0)), r))
        for r in range(n_dp)
    ]
    args = [dev, *pieces]
    alias = {}
    if prev is not None:
        specs.append(pl.BlockSpec(memory_space=pl.ANY))
        args.append(prev)
        alias = {n_dp + 1: 0}
    return pl.pallas_call(
        functools.partial(place_kernel, n_dp, per, off, last),
        grid_spec=pltpu.PrefetchScalarGridSpec(
            num_scalar_prefetch=1,
            grid=(n_dp, steps),
            in_specs=specs,
            out_specs=pl.BlockSpec((cols, rows), lambda s, j, d: (0, jnp.minimum(s * per + off + j, last))),
        ),
        out_shape=jax.ShapeDtypeStruct((cols, vocab_loc), jnp.float32),
        input_output_aliases=alias,
        cost_estimate=pl.CostEstimate(flops=n_dp * steps * rows * cols, bytes_accessed=8 * n_dp * steps * rows * cols, transcendentals=0),
        name="place",
    )(*args)


def solution(mesh):
    n_dp, n_tp = mesh.shape["dp"], mesh.shape["tp"]

    def swap(x, mask, axis="dp"):
        size = n_dp if axis == "dp" else n_tp
        return lax.ppermute(x, axis, [(i, i ^ mask) for i in range(size)])

    def local_step(hidden, labels, loss_mask, norm_gain, embed_table):
        n_seq, seq_len, hid = hidden.shape
        vocab_loc = embed_table.shape[0]
        tokens = n_seq * seq_len
        unit = 2 * VB * n_dp
        nblk = (vocab_loc + unit - 1) // unit * 2
        me = lax.axis_index("dp").astype(jnp.int32)
        plane = lax.axis_index("tp").astype(jnp.int32)
        dev = jnp.stack([me, plane])
        offset = plane * vocab_loc
        n_chip = n_dp // 2

        x_full = hidden.reshape(tokens, hid).astype(jnp.float32)
        gain32 = norm_gain.astype(jnp.float32)
        ints = jnp.stack([labels.reshape(tokens), loss_mask.reshape(tokens)]).astype(jnp.float32)
        mine = jnp.concatenate([x_full, jnp.pad(ints, ((0, 6), (0, hid - tokens)))])
        held = [mine] + [swap(mine, 2 * c) for c in range(1, n_chip)]
        prev, stats = None, []
        for g in range(n_chip):
            sib = swap(held[g], 1)
            res = logits_call(
                g, n_chip, vocab_loc, nblk, tokens, dev, held[g], sib, offset.reshape(1), gain32[None, :],
                embed_table if prev is None else e_dev, prev,
            )
            if prev is None:
                e_dev = res[4]
            prev = z, ut, lab = res[:3]
            stats.append(res[3])
        mask_all = jnp.concatenate([st[3] for st in stats]).reshape(n_dp, tokens)
        mask_count = jnp.sum(mask_all)

        stat = jnp.concatenate(stats, axis=1)[:3].reshape(3, n_dp, tokens)
        for axis, mask in (("dp", 1), ("dp", 2), ("dp", 4), ("tp", 1)):
            got = swap(stat, mask, axis)
            if axis == "dp":
                got = jnp.stack([got[:, r ^ mask] for r in range(n_dp)], axis=1)
            top = jnp.maximum(stat[0], got[0])
            stat = jnp.stack([
                top,
                stat[1] * jnp.exp(stat[0] - top) + got[1] * jnp.exp(got[0] - top),
                stat[2] + got[2],
            ])
        log_norm = stat[0] + jnp.log(stat[1])
        wide = lambda a: jnp.broadcast_to(a.reshape(-1)[:, None], (n_dp * tokens, 128))
        lse, wgt = wide(log_norm), wide(mask_all / mask_count)

        def after(x, *deps):
            return lax.optimization_barrier((x, *deps))[0]

        half = tokens // 2
        tb = half // 2
        odd_at = lambda i, d: (2 * (i // 3) + 1) * 3 + i % 3
        send_at = lambda i, d: (i // 2) * 8 + (1 - d[1]) * 2 + i % 2
        send_add = lambda i, d: (i // 2) * 4 + (1 - d[1]) * 2 + i % 2
        keep_at = lambda i, d: (i // 2) * 8 + d[1] * 2 + i % 2
        keep_add = lambda i, d: (i // 2) * 4 + d[1] * 2 + i % 2
        sent, turn = [], dev
        for c, (off, steps) in enumerate(CHUNKS):
            if c == len(CHUNKS) - 2:
                odd, = hidden_grad(turn, z, lse, wgt, lab, e_dev, 256, odd_at, 12, 1)
                turn = after(dev, odd)
                got = swap(odd, 1)
            if c == len(CHUNKS) - 1:
                away = hidden_grad(turn, z, lse, wgt, lab, e_dev, tb, send_at, 8, n_chip, got, send_add)
                turn = after(dev, away[0])
                back = [swap(p, 1, "tp") for p in away]
                kept = hidden_grad(turn, z, lse, wgt, lab, e_dev, tb, keep_at, 8, n_chip, got, keep_add)
                turn = after(dev, kept[0])
            pieces = embed_grad(turn, z, lse, wgt, lab, ut, off, steps, n_dp)
            sent.append((off, steps, [pieces[0]] + [swap(pieces[r], r) for r in range(1, n_dp)]))
            turn = after(dev, pieces[0])
        both = [k + b for k, b in zip(kept, back)]
        grad_norm = both[0]
        for c in range(1, n_chip):
            grad_norm = grad_norm + swap(both[c], 2 * c)

        x_half = lax.dynamic_slice_in_dim(hidden.reshape(tokens, hid), plane * half, half).astype(jnp.float32)
        inv_rms = lax.rsqrt(jnp.mean(x_half * x_half, axis=-1, keepdims=True) + EPSILON)
        x_hat = x_half * inv_rms
        a = grad_norm * gain32
        dh_half = inv_rms * (a - x_hat * jnp.mean(a * x_hat, axis=-1, keepdims=True))
        dh_other = swap(dh_half, 1, "tp")
        grad_hidden = jnp.where(plane == 0, jnp.concatenate([dh_half, dh_other]), jnp.concatenate([dh_other, dh_half]))
        own = jnp.sum(mask_all[0] * (log_norm[0] - stat[2, 0])) * (1.0 / n_tp)
        sums = jnp.concatenate([jnp.sum(grad_norm * x_hat, axis=0), own[None]])[None]
        for axis, mask in (("dp", 1), ("dp", 2), ("dp", 4), ("tp", 1)):
            sums = sums + swap(sums, mask, axis)

        out = None
        for off, steps, pieces in sent:
            ragged = n_dp * nblk * VB - (nblk // 2 - off - steps) * 2 * VB > vocab_loc
            out = (place if ragged else place_copy)(dev, pieces, out, off, steps, vocab_loc, nblk)

        grad_gain, loss_value = sums[0, :hid], sums[0, hid] / mask_count
        return loss_value, grad_hidden.reshape(n_seq, seq_len, hid), out.T, grad_gain

    return jax.shard_map(
        local_step,
        mesh=mesh,
        in_specs=(P("dp", None, None), P("dp", None), P("dp", None), P(), P("tp", None)),
        out_specs=(P(), P("dp", None, None), P("tp", "dp"), P()),
        check_vma=False,
    )
```
